32 devices in a mesh: section: 2 (over x), fsdp: 16 (over z, y, core).
Axes of the slice: x: 2, y: 2, z: 4, core: 2. Of those that a mesh axis runs over, the one named last changes fastest.
Arguments:
- tokens: bfloat16 [6, 512, 4096], P(None, 'fsdp'), may hold values from -6 to 6
- cotangent: bfloat16 [6, 512, 4096], P(None, 'fsdp'), may hold values from -6 to 6
- order: int32 [6], replicated, may hold values from 0 to 5, each once
- w_value: bfloat16 [2, 4096, 512], P('section', 'fsdp'), may hold values from -0.09375 to 0.09375
- w_out: bfloat16 [2, 512, 4096], P('section', None, 'fsdp'), may hold values from -0.25 to 0.25
- adapter_down: bfloat16 [2, 4096, 128], P('section', 'fsdp'), may hold values from -0.09375 to 0.09375
- adapter_up: bfloat16 [2, 128, 512], P('section', None, 'fsdp'), may hold values from -0.5 to 0.5
Outputs:
- input_grads: bfloat16 [2, 6, 512, 4096], P('section', None, 'fsdp')
- grad_down: float32 [2, 4096, 128], P('section', 'fsdp')
- grad_up: float32 [2, 128, 512], P('section', None, 'fsdp')
The draws below stay inside these ranges and needn't reach their ends.
Inputs may be any that keep to these rules, and one draw needn't show every extreme that they name: order names each microbatch 0 .. 5 exactly once.
All inputs are finite; a program needn't handle non-finite values.
Results may differ from the reference program's by a relative error of at most 0.02.
Values may be sent and summed in bfloat16 or wider, within the bound.
No kernel may reach another device: no remote copies, remote signals or barrier semaphores. Data moves between devices by JAX's collectives and lax.ppermute only.
A program may use at most 128 MiB of HBM per device.

```python
import jax
import jax.numpy as jnp
from jax import lax

D = 4096
HV = 512
R = 128
MICRO = 6
MB = 512
SECTIONS = 2


def with_spikes(entries, own_key, source, target, blocks, factor):
    def block_of(dim):
        return (jnp.arange(entries.shape[dim]) // (entries.shape[dim] // blocks)).reshape((-1,) + (1,) * (entries.ndim - 1 - dim))

    near = jax.random.permutation(own_key, blocks)[block_of(target)]
    second = (block_of(target) + blocks // 2) % blocks
    return jnp.where((block_of(source) == near) | (block_of(source) == second), factor * entries, entries)


def level_of(own_key, dims, pieces, least, top_value):
    gain, own = 1.0, jax.random.fold_in(own_key, 6)
    for dim, blocks in pieces:
        draws = jnp.exp(jax.random.uniform(jax.random.fold_in(own, dim), (blocks,), jnp.float32, least / len(pieces), top_value / len(pieces)))
        gain = gain * jnp.repeat(draws, dims[dim] // blocks).reshape([-1 if axis == dim else 1 for axis in range(len(dims))])
    return gain


def noise(rng, extent, width, most, cuts=(), kind=jnp.bfloat16):
    gain = level_of(rng, extent, cuts, -0.22, 0.18) if cuts else 1.0
    entries = jax.random.normal(rng, extent, jnp.float32) * width * gain
    return jnp.minimum(jnp.maximum(entries, -most), most).astype(kind)


def heavy_noise(rng, shape, spread, bound, shards, heavy, held_as=jnp.bfloat16):
    array = spread * jax.random.normal(rng, shape, jnp.float32)
    if shards:
        array = array * level_of(rng, shape, shards, -0.22, 0.18)
    return jnp.clip(with_spikes(array, jax.random.fold_in(rng, 3), *heavy), -bound, bound).astype(held_as)


def setup_inputs(seed: int = 0) -> dict:
    streams_of = jax.random.split(jax.random.key(seed), 8)
    return {
        "tokens": heavy_noise(streams_of[0], (MICRO, MB, D), 1.0, 6.0, ((1, 16),), (1, 2, 16, 2.0)),
        "cotangent": heavy_noise(streams_of[1], (MICRO, MB, D), 1.0, 6.0, ((1, 16),), (1, 2, 16, 2.0)),
        "order": jax.random.permutation(streams_of[2], MICRO).astype(jnp.int32),
        "w_value": noise(streams_of[3], (SECTIONS, D, HV), D ** -0.5, 0.09375, ((0, 2), (1, 16))),
        "w_out": noise(streams_of[4], (SECTIONS, HV, D), HV ** -0.5, 0.25, ((0, 2), (2, 16))),
        "adapter_down": noise(streams_of[5], (SECTIONS, D, R), D ** -0.5, 0.09375, ((0, 2), (1, 16))),
        "adapter_up": noise(streams_of[6], (SECTIONS, R, HV), R ** -0.5, 0.5, ((0, 2), (2, 16))),
    }


epsilon = 1e-05

def layer_forward(inputs, w_val, w_proj, a_down, a_up):
    widened = inputs.astype(jnp.float32)
    inverse = lax.rsqrt(lax.optimization_barrier(jnp.mean(widened * widened, axis=-1, keepdims=True)) + epsilon)
    normed = (widened * inverse).astype(jnp.bfloat16)
    low = jnp.dot(normed, a_down, preferred_element_type=jnp.float32).astype(jnp.bfloat16)
    values = (jnp.dot(normed, w_val, preferred_element_type=jnp.float32) + jnp.dot(low, a_up, preferred_element_type=jnp.float32)).astype(jnp.bfloat16)
    outputs = (widened + jnp.dot(values, w_proj, preferred_element_type=jnp.float32)).astype(jnp.bfloat16)
    return (outputs, normed, low, inverse)

def layer_backward(inputs, inverse, upstream, w_val, w_proj, a_down, a_up):
    d_values = jnp.dot(upstream, w_proj.T, preferred_element_type=jnp.float32).astype(jnp.bfloat16)
    d_low = jnp.dot(d_values, a_up.T, preferred_element_type=jnp.float32).astype(jnp.bfloat16)
    d_normed = jnp.dot(d_values, w_val.T, preferred_element_type=jnp.float32) + jnp.dot(d_low, a_down.T, preferred_element_type=jnp.float32)
    widened = inputs.astype(jnp.float32)
    project = lax.optimization_barrier(jnp.mean(d_normed * widened, axis=-1, keepdims=True))
    d_inputs = upstream.astype(jnp.float32) + inverse * (d_normed - widened * inverse * inverse * project)
    return (d_inputs.astype(jnp.bfloat16), d_values, d_low)

def reference(tokens, cotangent, order, w_value, w_out, adapter_down, adapter_up):
    current = tokens[order].reshape(MICRO * MB, D)
    stored = []
    for section_index in range(SECTIONS):
        stored.append(current)
        current = layer_forward(current, w_value[section_index], w_out[section_index], adapter_down[section_index], adapter_up[section_index])[0]
    upstream = cotangent[order].reshape(MICRO * MB, D)
    grads_in = [None] * SECTIONS
    down_grads = [None] * SECTIONS
    up_grads = [None] * SECTIONS
    for section_index in reversed(range(SECTIONS)):
        inputs = stored[section_index]
        unused, normed, low, inverse = layer_forward(inputs, w_value[section_index], w_out[section_index], adapter_down[section_index], adapter_up[section_index])
        d_inputs, d_values, d_low = layer_backward(inputs, inverse, upstream, w_value[section_index], w_out[section_index], adapter_down[section_index], adapter_up[section_index])
        down_grads[section_index] = jnp.dot(normed.T, d_low, preferred_element_type=jnp.float32)
        up_grads[section_index] = jnp.dot(low.T, d_values, preferred_element_type=jnp.float32)
        grads_in[section_index] = d_inputs.reshape(MICRO, MB, D)
        upstream = d_inputs
    return (jnp.stack(grads_in), jnp.stack(down_grads), jnp.stack(up_grads))
```

```python
import jax
import jax.numpy as jnp
from jax import lax
from jax.experimental import pallas as pl
from jax.experimental.pallas import tpu as pltpu
from jax.sharding import PartitionSpec as P

epsilon = 1e-05
lanes = 128
f32 = jnp.float32
bf16 = jnp.bfloat16


def dot(left, right):
    return jnp.dot(left, right, preferred_element_type=f32)


def dot_nt(left, right):
    return lax.dot_general(left, right, (((1,), (1,)), ((), ())), preferred_element_type=f32)


def dot_tn(left, right):
    return lax.dot_general(left, right, (((0,), (0,)), ((), ())), preferred_element_type=f32)


def sum_sections(part):
    sections = lax.axis_size("section")
    sent = part.astype(bf16)
    total = part
    for shift in range(1, sections):
        route = [(p, (p + shift) % sections) for p in range(sections)]
        total = total + lax.ppermute(sent, "section", route).astype(f32)
    return total


def sum_sections_wide(part):
    sections = lax.axis_size("section")
    total = part
    for shift in range(1, sections):
        route = [(p, (p + shift) % sections) for p in range(sections)]
        total = total + lax.ppermute(part, "section", route)
    return total


def spread(block, holder):
    sections = lax.axis_size("section")
    arrived = None
    for p in range(sections):
        if p != holder:
            got = lax.ppermute(block[p], "section", [(holder, p)])
            arrived = got if arrived is None else arrived + got
    return jnp.where(lax.axis_index("section") == holder, block[holder], arrived)


def places(n):
    depth = n // 4
    column = [[z] for z in range(depth)]
    size = 1
    while size < depth:
        grown = [list(held) for held in column]
        for base in range(0, depth, 2 * size):
            low, high = base + size - 1, base + size
            for t in range(size):
                grown[low - t] = column[low - t] + column[high]
                grown[high + t] = column[high + t] + column[low]
        column = grown
        size *= 2
    order = []
    for index in range(n):
        z, y, core = index // 4, index // 2 % 2, index % 2
        near = [h * 4 + y * 2 for h in column[z]] + [h * 4 + (1 - y) * 2 for h in column[z]]
        order.append([f + core for f in near] + [f + 1 - core for f in near])
    return order


def gather(block):
    n = lax.axis_size("fsdp")
    depth = n // 4
    z = lax.axis_index("fsdp") // 4

    def along(array, moves):
        route = [(a * 4 + rest, b * 4 + rest) for a, b in moves for rest in range(4)]
        return lax.ppermute(array, "fsdp", route)

    chunks = [block]
    size = 1
    while size < depth:
        payload = chunks[0] if len(chunks) == 1 else jnp.concatenate(chunks, axis=0)
        bases = range(0, depth, 2 * size)
        lows = [base + size - 1 for base in bases]
        far = along(payload, [m for a in lows for m in ((a, a + 1), (a + 1, a))])
        hop = far
        for t in range(1, size):
            hop = along(
                hop, [m for a in lows for m in ((a - t + 1, a - t), (a + t, a + t + 1))]
            )
            away = jnp.where(z % (2 * size) < size, size - 1 - z % size, z % size)
            far = jnp.where(away == t, hop, far)
        if size == 1:
            chunks = [jnp.concatenate([block, far], axis=0)]
        else:
            chunks.append(far)
        size *= 2
    other_y = [lax.ppermute(c, "fsdp", [(i, i ^ 2) for i in range(n)]) for c in chunks]
    near = chunks + other_y
    other_core = [lax.ppermute(c, "fsdp", [(i, i ^ 1) for i in range(n)]) for c in near]
    return near + other_core


def arrange_kernel(columns, tokens, cotangent, tokens_out, cotangent_out, inverse):
    rows, features = tokens.shape
    count = tokens_out.shape[1] // lanes
    for k in range(count):
        start = pl.multiple_of(columns[k] * lanes, lanes)
        tokens_out[:, k * lanes : (k + 1) * lanes] = tokens[:, pl.ds(start, lanes)]
        cotangent_out[:, k * lanes : (k + 1) * lanes] = cotangent[:, pl.ds(start, lanes)]
    total = jnp.zeros((rows, lanes), f32)
    for k in range(features // lanes):
        widened = tokens[:, k * lanes : (k + 1) * lanes].astype(f32)
        total = total + widened * widened
    mean = jnp.sum(total, axis=1, keepdims=True) / features
    inverse[...] = jnp.broadcast_to(lax.rsqrt(mean + epsilon), inverse.shape)


def arrange(tokens, cotangent, columns, part):
    rows, features = tokens.shape
    count = columns.shape[0]
    if part == lanes:
        whole = pl.BlockSpec(memory_space=pltpu.VMEM)
        half = jax.ShapeDtypeStruct((rows, count * part), bf16)
        x, u, inverse = pl.pallas_call(
            arrange_kernel,
            in_specs=[pl.BlockSpec(memory_space=pltpu.SMEM), whole, whole],
            out_specs=[whole, whole, whole],
            out_shape=[half, half, jax.ShapeDtypeStruct((rows, lanes), f32)],
        )(columns, tokens, cotangent)
        return x, u, inverse[:, :1]
    pick = lambda a: jnp.take(a.reshape(rows, -1, part), columns, axis=1).reshape(rows, -1)
    widened = tokens.astype(f32)
    inverse = lax.rsqrt(jnp.mean(widened * widened, axis=1, keepdims=True) + epsilon)
    return pick(tokens), pick(cotangent), inverse


def restore_kernel(order, places_of, where, mine, other, out):
    slots, rows, features = out.shape
    count = mine.shape[1] // lanes
    first = where[0] == 0
    for f in range(count):
        start = pl.multiple_of(places_of[f] * lanes, lanes)
        for j in range(slots):
            top = pl.multiple_of(order[j] * rows, rows)
            a = mine[pl.ds(top, rows), pl.ds(start, lanes)]
            b = other[pl.ds(top, rows), pl.ds(start, lanes)]
            out[j, :, 2 * f * lanes : (2 * f + 1) * lanes] = jnp.where(first, a, b)
            out[j, :, (2 * f + 1) * lanes : (2 * f + 2) * lanes] = jnp.where(first, b, a)


def restore(mine, arrived, order, places_of, shape, part):
    sections, position = lax.axis_size("section"), lax.axis_index("section")
    slots, rows, features = shape
    if sections == 2 and part == lanes:
        whole = pl.BlockSpec(memory_space=pltpu.VMEM)
        scalar = pl.BlockSpec(memory_space=pltpu.SMEM)
        return pl.pallas_call(
            restore_kernel,
            in_specs=[scalar, scalar, scalar, whole, whole],
            out_specs=whole,
            out_shape=jax.ShapeDtypeStruct(shape, bf16),
        )(order, places_of, position.reshape(1), mine, arrived)
    parts = arrived.reshape(sections, slots * rows, -1, part)
    parts = jnp.take(parts, places_of, axis=2).transpose(1, 2, 0, 3)
    return jnp.take(parts.reshape(shape), order, axis=0)


def body(tokens, cotangent, order, w_value, w_out, adapter_down, adapter_up):
    sections, position = lax.axis_size("section"), lax.axis_index("section")
    n, index = lax.axis_size("fsdp"), lax.axis_index("fsdp")
    last = sections - 1
    slots, rows, features = tokens.shape
    width, rank = w_value.shape[2], adapter_down.shape[2]
    share = features // n
    part = share // sections
    share_up = width // n

    table = places(n)
    held = jnp.asarray(table, jnp.int32)[index]
    back = jnp.asarray([[t.index(f) for f in range(n)] for t in table], jnp.int32)[index]
    columns = held * sections + position

    forward_block = jnp.concatenate([w_value[0], adapter_down[0]], axis=1)
    output_block = w_out[0].T
    up_rows = adapter_up[0].T
    packed = sections == 2 and 2 * share_up <= part
    weights = []
    for g in range(sections):
        a = forward_block.reshape(sections, part, width + rank)
        b = output_block.reshape(sections, part, width)
        if packed and g == 0:
            early = jnp.pad(up_rows, ((0, part - share_up), (0, 0)))
            late = jnp.pad(up_rows, ((share_up, part - 2 * share_up), (0, 0)))
            shape = (sections, part, rank)
            a = jnp.concatenate([a, jnp.broadcast_to(early, shape)], axis=2)
            b = jnp.concatenate([b, jnp.broadcast_to(late, shape)], axis=2)
        a = spread(a, g)
        b = spread(b, last - g)
        if packed and g == 0:
            ups = a[:, width + rank :] + b[:, width:]
            piece = jnp.concatenate([a[:, : width + rank], b[:, :width], ups], axis=1)
        else:
            piece = jnp.concatenate([a, b], axis=1)
        weights.append(jnp.concatenate(gather(piece), axis=0))
    cat = [w[:, : width + rank] for w in weights]
    out_rows = [weights[last - l][:, width + rank : 2 * width + rank] for l in range(sections)]
    if packed:
        ups = weights[0][:, 2 * width + rank :].reshape(n, part, rank)
        ups = jnp.take(ups, back, axis=0)
        up_t = [
            ups[:, l * share_up : (l + 1) * share_up].reshape(width, rank) for l in range(sections)
        ]
    else:
        ups = lax.all_gather(adapter_up, "section", axis=0, tiled=True)
        ups = lax.all_gather(ups, "fsdp", axis=2, tiled=True)
        up_t = [ups[l].T for l in range(sections)]

    x0, upstream, inverse0 = arrange(
        tokens.reshape(-1, features), cotangent.reshape(-1, features), columns, part
    )

    x, inverse, sums, low, d_values = [x0], [inverse0], [], [], [None] * sections
    for l in range(last):
        share_sum = dot(x[l], cat[l])
        if l == 0:
            both = jnp.concatenate([share_sum, dot(upstream, out_rows[last])], axis=1)
            both = sum_sections(both)
            d_values[last] = both[:, width + rank :].astype(bf16)
            sums.append(both[:, : width + rank])
        else:
            square = jnp.sum(x[l].astype(f32) ** 2, axis=1)
            mean = sum_sections_wide(square)[:, None] / features
            inverse.append(lax.rsqrt(mean + epsilon))
            sums.append(sum_sections(share_sum))
        low.append((sums[l][:, width:] * inverse[l]).astype(bf16))
        values = (sums[l][:, :width] * inverse[l] + dot_nt(low[l], up_t[l])).astype(bf16)
        x.append((x[l].astype(f32) + dot_nt(values, out_rows[l])).astype(bf16))

    d_low, grads = [None] * sections, [None] * sections
    for l in reversed(range(sections)):
        if l < last:
            d_values[l] = sum_sections(dot(upstream, out_rows[l])).astype(bf16)
        d_low[l] = dot(d_values[l], up_t[l]).astype(bf16)
        d_both = jnp.concatenate([d_values[l], d_low[l]], axis=1)
        d_normed = dot_nt(d_both, cat[l])
        widened = x[l].astype(f32)
        if l == last:
            square = jnp.sum(widened * widened, axis=1)
            product = jnp.sum(d_normed * widened, axis=1)
            square, product = sum_sections_wide(jnp.stack([square, product]))
            inverse.append(lax.rsqrt(square[:, None] / features + epsilon))
            project = product[:, None] / features
            share_low = sum_sections(dot(x[l], cat[l][:, width:]))
            low.append((share_low * inverse[l]).astype(bf16))
        else:
            project = jnp.sum(d_both.astype(f32) * sums[l], axis=1, keepdims=True) / features
        upstream = upstream.astype(f32) + inverse[l] * (
            d_normed - widened * inverse[l] * inverse[l] * project
        )
        upstream = upstream.astype(bf16)
        grads[l] = upstream

    if sections == 2:
        mine = jnp.where(position == 0, grads[0], grads[1])
        sent = jnp.where(position == 0, grads[1], grads[0])
        arrived = lax.ppermute(sent, "section", [(0, 1), (1, 0)])
    else:
        stacked = jnp.stack(grads)
        mine = lax.dynamic_index_in_dim(stacked, position, 0, keepdims=False)
        arrived = lax.dynamic_update_index_in_dim(stacked, mine, position, 0)
        for shift in range(1, sections):
            route = [(p, (p + shift) % sections) for p in range(sections)]
            sent = lax.dynamic_index_in_dim(stacked, (position + shift) % sections, 0, False)
            got = lax.ppermute(sent, "section", route)
            arrived = lax.dynamic_update_index_in_dim(
                arrived, got, (position - shift) % sections, 0
            )
    input_grads = restore(mine, arrived, order, back, tokens.shape, part)

    downs = [dot_tn(x[l], (inverse[l] * d_low[l].astype(f32)).astype(bf16)) for l in range(sections)]
    choose = lambda items: lax.dynamic_index_in_dim(jnp.stack(items), position, 0, keepdims=False)
    up = dot_tn(choose(d_values), choose(low)).reshape(n, share_up, rank)
    up = jnp.take(up, held, axis=0)
    total = jnp.concatenate([d.reshape(n, part, rank) for d in downs] + [up], axis=1)
    for bit in (1, 2):
        half = total.shape[0] // 2
        sent = total[half:].astype(bf16)
        got = lax.ppermute(sent, "fsdp", [(i, i ^ bit) for i in range(n)])
        total = total[:half] + got.astype(f32)
    depth = n // 4
    column = jnp.asarray([[f // 4 for f in t[:depth]] for t in table], jnp.int32)[index]
    own = total[0]
    for far in range(1, depth):
        wanted = jnp.argmax(column == ((index // 4) ^ far))
        sent = lax.dynamic_index_in_dim(total, wanted, 0, keepdims=False).astype(bf16)
        got = lax.ppermute(sent, "fsdp", [(i, i ^ (far * 4)) for i in range(n)])
        own = own + got.astype(f32)
    up_grad = own[sections * part :]
    own = own[: sections * part].reshape(sections, part, rank)
    mine = lax.dynamic_index_in_dim(own, position, 0, keepdims=False)
    down_grad = lax.dynamic_update_index_in_dim(own, mine, position, 0)
    for shift in range(1, sections):
        route = [(p, (p + shift) % sections) for p in range(sections)]
        sent = lax.dynamic_index_in_dim(own, (position + shift) % sections, 0, keepdims=False)
        got = lax.ppermute(sent.astype(bf16), "section", route).astype(f32)
        down_grad = lax.dynamic_update_index_in_dim(down_grad, got, (position - shift) % sections, 0)
    return (input_grads[None], down_grad.reshape(1, share, rank), up_grad.T[None])


def solution(mesh):
    return jax.shard_map(
        body,
        mesh=mesh,
        in_specs=(
            P(None, "fsdp", None),
            P(None, "fsdp", None),
            P(),
            P("section", "fsdp", None),
            P("section", None, "fsdp"),
            P("section", "fsdp", None),
            P("section", None, "fsdp"),
        ),
        out_specs=(
            P("section", None, "fsdp", None),
            P("section", "fsdp", None),
            P("section", None, "fsdp"),
        ),
        check_vma=False,
    )
```
